256 devices in a mesh: expert: 16 (over z, core), shard: 16 (over y, x).
Axes of the slice: x: 4, y: 4, z: 8, core: 2. Of those that a mesh axis runs over, the one named last changes fastest.
Arguments:
- w_down: float32 [64, 1024, 2048], P('expert', None, 'shard'), may hold values from -0.25 to 0.25
- avg_down: float32 [64, 1024, 2048], P('expert', None, 'shard'), may hold values from -0.1875 to 0.1875
- mix_share: float32 [64], P('expert'), may hold values from 0.2 to 0.8
- router_weight: float32 [2048, 64], P('shard', 'expert'), may hold values from -0.125 to 0.125
- router_gain: float32 [2048], P('shard'), may hold values from 0.25 to 1.75
Outputs:
- serve_down: bfloat16 [64, 1024, 2048], P('expert')
- scale_down: float32 [64, 1024], P('expert')
- serve_router: bfloat16 [2048, 64], replicated
The draws below stay inside these ranges and needn't reach their ends.
All inputs are finite; a program needn't handle non-finite values. Where the reference program divides by a largest or mean magnitude, that divisor is 1e-20 or more.
Results may differ from the reference program's by a relative error of at most 0.001.
Values may be sent and summed in bfloat16 or wider, within the bound.
No kernel may reach another device: no remote copies, remote signals or barrier semaphores. Data moves between devices by JAX's collectives and lax.ppermute only.
A program may use at most 128 MiB of HBM per device.

```python
import jax
import jax.numpy as jnp

EXPERTS = 64
D_MODEL = 2048
D_EXPERT = 1024


def strengthened(values, stream_key, source, target, blocks, factor):
    def block_of(dim):
        return (jnp.arange(values.shape[dim]) // (values.shape[dim] // blocks)).reshape((-1,) + (1,) * (values.ndim - 1 - dim))

    one_side = jax.random.permutation(stream_key, blocks)[block_of(target)]
    second = (block_of(target) + blocks // 2) % blocks
    return jnp.where((block_of(source) == one_side) | (block_of(source) == second), factor * values, values)


def block_levels(key, extent, pieces, low, largest):
    level, own = 1.0, jax.random.fold_in(key, 6)
    for position, blocks in pieces:
        steps = jnp.exp(jax.random.uniform(jax.random.fold_in(own, position), (blocks,), jnp.float32, low / len(pieces), largest / len(pieces)))
        level = level * jnp.repeat(steps, extent[position] // blocks).reshape([-1 if axis == position else 1 for axis in range(len(extent))])
    return level


def centred(key, dims, width, most, split=(), held_as=jnp.bfloat16):
    values = width * jax.random.normal(key, dims, jnp.float32)
    if split:
        values = values * block_levels(key, dims, split, -0.22, 0.18)
    return jnp.clip(values, -most, most).astype(held_as)


def gaussian_with(key, dims, width, bound, split, heavy, kind=jnp.bfloat16):
    result = width * jax.random.normal(key, dims, jnp.float32)
    if split:
        result = result * block_levels(key, dims, split, -0.22, 0.18)
    return jnp.clip(strengthened(result, jax.random.fold_in(key, 3), *heavy), -bound, bound).astype(kind)


def setup_inputs(seed: int = 0) -> dict:
    key_list = jax.random.split(jax.random.key(seed), 6)
    return {
        "w_down": gaussian_with(key_list[0], (EXPERTS, D_EXPERT, D_MODEL), D_EXPERT ** -0.5, 0.25, ((0, 16), (2, 16)), (2, 1, 16, 2.0), jnp.float32),
        "avg_down": centred(key_list[1], (EXPERTS, D_EXPERT, D_MODEL), D_EXPERT ** -0.5, 0.1875, ((0, 16), (2, 16)), jnp.float32),
        "mix_share": jnp.clip(0.2 + 0.6 * jax.random.uniform(key_list[2], (EXPERTS,), jnp.float32) ** block_levels(key_list[2], (EXPERTS,), ((0, 16),), -0.2, 0.2), 0.2, 0.8),
        "router_weight": centred(key_list[3], (D_MODEL, EXPERTS), D_MODEL ** -0.5, 0.125, ((0, 16), (1, 16)), jnp.float32),
        "router_gain": jnp.clip(1.0 + 0.15 * jax.random.normal(key_list[4], (D_MODEL,), jnp.float32), 0.25, 1.75),
    }


def reference(w_down, avg_down, mix_share, router_weight, router_gain):
    fresh_down = mix_share[:, None, None] * w_down + (1.0 - mix_share[:, None, None]) * avg_down
    scale_down = jnp.sum(jnp.abs(fresh_down), axis=2) / D_MODEL
    serve_down = (fresh_down / jnp.expand_dims(scale_down, 2)).astype(jnp.bfloat16)
    serve_router = (router_weight * router_gain[:, None]).astype(jnp.bfloat16)
    return serve_down, scale_down, serve_router
```

```python
import jax
import jax.numpy as jnp
from jax import lax
from jax.experimental import pallas as pl
from jax.experimental.pallas import tpu as pltpu
from jax.sharding import PartitionSpec as P

D_MODEL = 2048
SIDE = 4
LANES = 128


def moved(value, dim, step):
    pairs = []
    for y in range(SIDE):
        for x in range(SIDE):
            tx, ty = ((x + step) % SIDE, y) if dim == 0 else (x, (y + step) % SIDE)
            pairs.append((y * SIDE + x, ty * SIDE + tx))
    return lax.ppermute(value, "shard", pairs)


def swapped(value, axis, bit):
    n = lax.axis_size(axis)
    return lax.ppermute(value, axis, [(i, i ^ bit) for i in range(n)])


def plane_sum(value):
    for dim in (0, 1):
        near = moved(value, dim, 1) + moved(value, dim, -1)
        value = (value + moved(value, dim, 2)) + near
    return value


def plan():
    sends = []

    def send(e, n, i, j, dim, step, half=None):
        first = (0 if e < 2 else 1) == dim
        se, sn = (e, n) if half is None else (e + half, 1)
        far = (i + step, j) if first else (i, j + step)
        key = (se, sn) + tuple(2 if abs(p) == 2 else p for p in far)
        sends.append((dim, step, (e, n, i, j), half, key))

    def dims(e):
        return (0, 1) if e < 2 else (1, 0)

    signs = ((1, 0), (-1, 1))
    for k in (0, 1):
        for e in (0, 2):
            for s, _ in signs:
                send(e, 2, 0, 0, dims(e)[k], s)
    for e in (0, 2):
        for s, h in signs:
            send(e, 2, s, 0, dims(e)[0], s, h)
    for i in (1, -1):
        for e in (0, 2):
            for s, _ in signs:
                send(e, 2, i, 0, dims(e)[1], s)
    for h in (0, 1):
        for e in (0, 2):
            for s, _ in signs:
                send(e + h, 1, 2, 0, dims(e)[1], s)
    for i in (0, 1, -1):
        for e in (0, 2):
            for s, h in signs:
                send(e, 2, i, s, dims(e)[1], s, h)
    for e in (0, 2):
        for s, h in signs:
            send(e + h, 1, 2, s, dims(e)[1], s)
    return sends


def placed(pieces, out, shape):
    n = len(pieces)

    def kernel(*refs):
        out_ref, sems = refs[-2], refs[-1]
        index = lax.axis_index("shard")
        copies = []
        for k, ((e, count, i, j), ref) in enumerate(zip(pieces, refs)):
            dx, dy = (i, j) if e < 2 else (j, i)
            x = (index + (SIDE - dx)) & (SIDE - 1)
            y = (index // SIDE + (SIDE - dy)) & (SIDE - 1)
            start = pl.multiple_of((y * SIDE + x) * LANES, LANES)
            copies.append(
                pltpu.make_async_copy(
                    ref,
                    out_ref.at[pl.ds(e, count), :, pl.ds(start, LANES)],
                    sems.at[k],
                )
            )
        for copy in copies:
            copy.start()
        for copy in copies:
            copy.wait()

    operands = [pltpu.with_memory_space_constraint(v, pltpu.VMEM) for v in pieces.values()]
    specs = [pl.BlockSpec(memory_space=pltpu.VMEM)] * n
    if out is not None:
        operands.append(pltpu.with_memory_space_constraint(out, pltpu.HBM))
        specs.append(pl.BlockSpec(memory_space=pltpu.HBM))
    size = sum(2 * v.size for v in pieces.values())
    return pl.pallas_call(
        kernel,
        out_shape=pltpu.HBM(shape, jnp.bfloat16),
        in_specs=specs,
        out_specs=pl.BlockSpec(memory_space=pltpu.HBM),
        scratch_shapes=[pltpu.SemaphoreType.DMA((n,))],
        input_output_aliases={} if out is None else {n: 0},
        cost_estimate=pl.CostEstimate(flops=size, bytes_accessed=2 * size, transcendentals=0),
        compiler_params=pltpu.CompilerParams(vmem_limit_bytes=8 << 20),
        name=f"placed_{n}",
    )(*operands)


def router_laid_out(blocks):
    experts, shards, rows, lanes = blocks.shape

    def kernel(in_ref, out_ref):
        e, s = lax.axis_index("expert"), lax.axis_index("shard")
        for m in range(shards):
            column = [
                in_ref[k ^ e, m ^ s].astype(jnp.float32) for k in range(experts)
            ]
            out_ref[:, m * lanes : (m + 1) * lanes] = jnp.concatenate(column, 0).astype(
                out_ref.dtype
            )

    return pl.pallas_call(
        kernel,
        out_shape=jax.ShapeDtypeStruct((experts * rows, shards * lanes), blocks.dtype),
        compiler_params=pltpu.CompilerParams(vmem_limit_bytes=4 << 20),
        name="router_laid_out",
    )(blocks)


GROUPS = (12, 24, 36, 44)
ROUTER_AT = (4, 8, 12, 16, 20, 24, 28, 32)


def gathered_down(pairs, router):
    have = {(2 * k, 2, 0, 0): pair for k, pair in enumerate(pairs)}
    fresh = dict(have)
    shape = (2 * len(pairs), pairs[0].shape[1], SIDE * SIDE * LANES)
    sends = plan()
    out = None
    steps = [("shard", bit) for bit in (1, 2, 4, 8)] + [("expert", bit) for bit in (1, 2, 4, 8)]
    other = None
    router = router[None, None]
    for n, (dim, step, source, half, target) in enumerate(sends):
        if n in ROUTER_AT:
            if other is not None:
                have[source], other = lax.optimization_barrier((have[source], other))
                router = jnp.concatenate([router, other], axis)
            axis, bit = steps.pop(0)
            other = swapped(router, axis, bit)
            axis = 1 if axis == "shard" else 0
        value = have[source]
        if half is not None:
            value = value[half : half + 1]
        have[target] = fresh[target] = moved(value, dim, step)
        if n + 1 in GROUPS:
            out = placed(fresh, out, shape)
            fresh = {}
    return out, router_laid_out(jnp.concatenate([router, other], axis))


def body(w_down, avg_down, mix_share, router_weight, router_gain):
    share = mix_share[:, None, None]
    fresh_down = share * w_down + (1.0 - share) * avg_down
    scale_down = plane_sum(jnp.sum(jnp.abs(fresh_down), axis=2)) / D_MODEL
    pairs = [
        (fresh_down[e : e + 2] / scale_down[e : e + 2, :, None]).astype(jnp.bfloat16)
        for e in (0, 2)
    ]
    part_router = (router_weight * router_gain[:, None]).astype(jnp.bfloat16)
    serve_down, router = gathered_down(pairs, part_router.T)
    return (serve_down, scale_down, router.T)


def solution(mesh):
    return jax.shard_map(
        body,
        mesh=mesh,
        in_specs=(
            P("expert", None, "shard"),
            P("expert", None, "shard"),
            P("expert"),
            P("shard", "expert"),
            P("shard"),
        ),
        out_specs=(P("expert", None, None), P("expert", None), P()),
        check_vma=False,
    )
```
